32 devices in a mesh: grp: 4 (over x, core), sub: 8 (over z, y).
Axes of the slice: x: 2, y: 2, z: 4, core: 2. Of those that a mesh axis runs over, the one named last changes fastest.
Arguments:
- fine_res: float32 [3, 131072], P(None, ('grp', 'sub'))
- node_map: int32 [2, 131072], P(None, ('grp', 'sub')), may hold values from 0 to 16383, as said below
- connect: int32 [4, 32768], P(None, 'sub'), may hold values from 0 to 16383, as said below
- grads: float32 [3, 3, 32768], P(None, None, 'sub'), may hold values from -6 to 6
- moduli: float32 [2, 32768], P(None, 'sub'), may hold values from 0.2 to 2
- mass: float32 [16384], P('sub'), may hold values from 0.5 to 4
Outputs:
- correction: float32 [3, 131072], P(None, ('grp', 'sub'))
The draws below stay inside these ranges and needn't reach their ends.
Inputs may be any that keep to these rules, and one draw needn't show every extreme that they name: `node_map`: fine nodes 4096 * b to 4096 * (b + 1) - 1 lie in column c = b % 8; both their entries are coarse nodes c * 2048 to (c + 1) * 2048 - 1 or the first 1024 nodes of column c + 1; the two entries are equal at vertices. `connect`: tetrahedra c * 4096 to (c + 1) * 4096 - 1 lie in column c; their nodes are coarse nodes of column c or the first 1024 nodes of column c + 1.
All inputs are finite; a program needn't handle non-finite values.
Results may differ from the reference program's by a relative error of at most 0.0001.
Values sent between devices are 32-bit elements; how exact they have to be, the bound alone decides.
A program may use at most 64 MiB of HBM per device.

```python
import math
import jax
import jax.numpy as jnp

CN = 2048
CI = 1024
CE = 4096
FN = 4096
ITERS = 3
CNODES = 16384
CELEMS = 32768
FNODES = 131072
N_SUB = 8


def pick_nodes(key, count, column):
    keys = jax.random.split(key, 3)
    own = jax.random.randint(keys[0], (count,), 0, CN, dtype=jnp.int32)
    shared = jax.random.randint(keys[1], (count,), 0, CI, dtype=jnp.int32)
    coin = jax.random.randint(keys[2], (count,), 0, 100, dtype=jnp.int32)
    use_next = (coin < 20) & (column < N_SUB - 1)
    return jnp.where(use_next, (column + 1) * CN + shared, column * CN + own).astype(jnp.int32)


def draw_fine_res(key, part):
    column = jnp.arange(FNODES, dtype=jnp.int32) // FN % N_SUB
    scale = 1.0 + 2.0 * column.astype(jnp.float32) / max(N_SUB - 1, 1)
    values = jax.random.normal(key, (3, FNODES), jnp.float32) * scale[None, :]
    return values


def draw_node_map(key, part):
    column = jnp.arange(FNODES, dtype=jnp.int32) // FN % N_SUB
    keys = jax.random.split(jax.random.fold_in(key, 11), 3)
    first = pick_nodes(keys[0], FNODES, column)
    second = pick_nodes(keys[1], FNODES, column)
    coin = jax.random.randint(keys[2], (FNODES,), 0, 8, dtype=jnp.int32)
    second = jnp.where(coin == 0, first, second)
    return jnp.stack([first, second]).astype(jnp.int32)


def draw_connect(key, part):
    column = jnp.arange(CELEMS, dtype=jnp.int32) // CE
    keys = jax.random.split(jax.random.fold_in(key, 23), 4)
    return jnp.stack([pick_nodes(keys[corner], CELEMS, column) for corner in range(4)]).astype(jnp.int32)


def block_levels(own_key, extent, cuts, low, largest):
    gain, own = 1.0, jax.random.fold_in(own_key, 6)
    for axis_at, shards_of in cuts:
        draws = jnp.exp(jax.random.uniform(jax.random.fold_in(own, axis_at), (shards_of,), jnp.float32, low / len(cuts), largest / len(cuts)))
        gain = gain * jnp.repeat(draws, extent[axis_at] // shards_of).reshape([-1 if axis == axis_at else 1 for axis in range(len(extent))])
    return gain


def normal_values(key, shape, spread, most, shards=(), held_as=jnp.bfloat16):
    drawn = jax.random.normal(key, shape, jnp.float32) * spread
    if len(shards) > 0:
        drawn = block_levels(key, shape, shards, -0.22, 0.18) * drawn
    return jnp.clip(drawn, min=-most, max=most).astype(held_as)


def setup_inputs(seed: int = 0) -> dict:
    streams_of = jax.random.split(jax.random.key(seed), 7)
    fine_res = draw_fine_res(jax.random.fold_in(streams_of[6], 71), 0)
    node_map = draw_node_map(jax.random.fold_in(streams_of[6], 71), 0)
    connect = draw_connect(jax.random.fold_in(streams_of[6], 71), 0)
    grads = normal_values(streams_of[3], (3, 3, CELEMS), 1.0, 6.0, ((2, 8),), jnp.float32)
    moduli = jnp.clip(jnp.exp(math.log(2.0) - 2.3025851 * jax.random.uniform(streams_of[4], (2, CELEMS), jnp.float32) ** block_levels(streams_of[4], (2, CELEMS), ((1, 8),), -0.2, 0.2)), 0.2, 2.0)
    mass = jnp.clip(jnp.exp(math.log(4.0) - 2.0794415 * jax.random.uniform(streams_of[5], (CNODES,), jnp.float32) ** block_levels(streams_of[5], (CNODES,), ((0, 8),), -0.2, 0.2)), 0.5, 4.0)
    return {"fine_res": fine_res, "node_map": node_map, "connect": connect, "grads": grads, "moduli": moduli, "mass": mass}


def element_forces(field, connect, grads, moduli, count):
    last = -(grads[:, 0] + grads[:, 1] + grads[:, 2])
    shape_grads = (grads[:, 0], grads[:, 1], grads[:, 2], last)
    displ_grad = jnp.zeros((3, 3, connect.shape[1]), jnp.float32)
    for corner in range(4):
        moved = jnp.take(field, connect[corner], axis=1)
        displ_grad = displ_grad + moved[:, None, :] * shape_grads[corner][None, :, :]
    strain = 0.5 * (displ_grad + jnp.transpose(displ_grad, (1, 0, 2)))
    trace = strain[0, 0] + strain[1, 1] + strain[2, 2]
    identity = jnp.eye(3, dtype=jnp.float32)[:, :, None]
    stress = 2.0 * moduli[1] * strain + (moduli[0] * trace) * identity
    forces = jnp.zeros((3, count), jnp.float32)
    for corner in range(4):
        nodal = jnp.sum(stress * shape_grads[corner][None, :, :], axis=1)
        forces = forces.at[:, connect[corner]].add(nodal)
    return forces


def operate(field, connect, grads, moduli, mass):
    return mass[None, :] * field + element_forces(field, connect, grads, moduli, field.shape[1])


def reference(fine_res, node_map, connect, grads, moduli, mass):
    total = mass.shape[0]
    half = 0.5 * fine_res
    rhs = jnp.zeros((3, total), jnp.float32).at[:, node_map[0]].add(half).at[:, node_map[1]].add(half)
    solution = jnp.zeros((3, total), jnp.float32)
    residual = rhs
    direction = rhs
    norm_now = jnp.sum(residual * residual)
    for step in range(ITERS):
        image = operate(direction, connect, grads, moduli, mass)
        alpha = norm_now / jnp.sum(direction * image)
        solution = solution + alpha * direction
        residual = residual - alpha * image
        norm_next = jnp.sum(residual * residual)
        direction = residual + (norm_next / norm_now) * direction
        norm_now = norm_next
    return 0.5 * (jnp.take(solution, node_map[0], axis=1) + jnp.take(solution, node_map[1], axis=1))
```

```python
import functools

import jax
import jax.numpy as jnp
from jax import lax
from jax.experimental import pallas as pl
from jax.experimental.pallas import tpu as pltpu
from jax.sharding import PartitionSpec as P

CI = 1024
ITERS = 3
LANES = 128
TILE = 512
F32 = jnp.float32
BF16 = jnp.bfloat16
NT = (((1,), (1,)), ((), ()))


def split(value):
    high = value.astype(BF16)
    return high, (value - high.astype(F32)).astype(BF16)


def hots(index, rows):
    lane = index & (LANES - 1)
    row = index // LANES
    width = index.shape[1]
    lane_hot = jnp.where(lax.broadcasted_iota(jnp.int32, (LANES, width), 0) == lane, 1.0, 0.0).astype(BF16)
    row_hot = lax.broadcasted_iota(jnp.int32, (rows, width), 0) == row
    return lane_hot, row_hot


def pick(parts, lane_hot, row_hot, rows):
    got = jnp.dot(parts, lane_hot, preferred_element_type=F32)
    half = 3 * rows
    got = got[:half] + got[half:]
    return [
        jnp.sum(jnp.where(row_hot, got[d * rows : (d + 1) * rows], 0.0), axis=0, keepdims=True)
        for d in range(3)
    ]


def spread(values, lane_hot, row_hot):
    placed = []
    for value in values:
        placed.append(jnp.where(row_hot, value, 0.0))
    placed = jnp.concatenate(placed, axis=0)
    parts = jnp.concatenate(split(placed), axis=0)
    got = lax.dot_general(parts, lane_hot, NT, preferred_element_type=F32)
    half = got.shape[0] // 2
    return got[:half] + got[half:]


def field_parts(field_ref, rows):
    field = field_ref[...].reshape(3 * rows, LANES)
    return jnp.concatenate(split(field), axis=0)


def restrict_kernel(fine_ref, map_ref, out_ref, *, rows, nodes):
    base = lax.axis_index("sub") * nodes
    total = jnp.zeros((3 * rows, LANES), F32)
    for at in range(0, fine_ref.shape[1], TILE):
        values = [0.5 * fine_ref[d : d + 1, at : at + TILE] for d in range(3)]
        for k in range(2):
            lane_hot, row_hot = hots(map_ref[k : k + 1, at : at + TILE] - base, rows)
            total = total + spread(values, lane_hot, row_hot)
    out_ref[...] = total.reshape(3, rows, LANES)


def prolong_kernel(field_ref, map_ref, out_ref, *, rows, nodes):
    base = lax.axis_index("sub") * nodes
    parts = field_parts(field_ref, rows)
    for at in range(0, out_ref.shape[1], TILE):
        both = []
        for k in range(2):
            lane_hot, row_hot = hots(map_ref[k : k + 1, at : at + TILE] - base, rows)
            both.append(pick(parts, lane_hot, row_hot, rows))
        for d in range(3):
            out_ref[d : d + 1, at : at + TILE] = 0.5 * (both[0][d] + both[1][d])


def force_kernel(field_ref, conn_ref, grads_ref, moduli_ref, out_ref, *, rows, nodes):
    base = lax.axis_index("sub") * nodes
    parts = field_parts(field_ref, rows)
    total = jnp.zeros((3 * rows, LANES), F32)
    for at in range(0, conn_ref.shape[1], TILE):
        cut = slice(at, at + TILE)
        grad = [[grads_ref[i, a : a + 1, cut] for i in range(3)] for a in range(3)]
        grad.append([-(grad[0][i] + grad[1][i] + grad[2][i]) for i in range(3)])
        first = moduli_ref[0:1, cut]
        second = moduli_ref[1:2, cut]
        hot = [hots(conn_ref[a : a + 1, cut] - base, rows) for a in range(4)]
        moved = [pick(parts, hot[a][0], hot[a][1], rows) for a in range(4)]
        h = [[sum(moved[a][i] * grad[a][j] for a in range(4)) for j in range(3)] for i in range(3)]
        bulk = first * (h[0][0] + h[1][1] + h[2][2])
        stress = [[second * (h[i][j] + h[j][i]) for j in range(3)] for i in range(3)]
        for i in range(3):
            stress[i][i] = stress[i][i] + bulk
        for a in range(4):
            nodal = [sum(stress[i][j] * grad[a][j] for j in range(3)) for i in range(3)]
            total = total + spread(nodal, hot[a][0], hot[a][1])
    out_ref[...] = total.reshape(3, rows, LANES)


def call(kernel, shape, *args, **sizes):
    return pl.pallas_call(
        functools.partial(kernel, **sizes),
        out_shape=jax.ShapeDtypeStruct(shape, F32),
        compiler_params=pltpu.CompilerParams(vmem_limit_bytes=48 * 1024 * 1024),
    )(*args)


def shifted(shard, axis, by):
    size = lax.axis_size(axis)
    pairs = [(i, i + by) for i in range(size) if 0 <= i + by < size]
    return lax.ppermute(shard, axis, pairs)


def joined(field, own_rows, shared_rows):
    carried = shifted(field[:, own_rows:], "sub", 1)
    upper = shifted(field[:, :shared_rows], "sub", -1)
    return jnp.concatenate(
        [
            field[:, :shared_rows] + carried,
            field[:, shared_rows:own_rows],
            field[:, own_rows:] + upper,
        ],
        axis=1,
    )


def body(fine_res, node_map, connect, grads, moduli, mass):
    nodes = mass.shape[0]
    own = nodes // LANES
    shared = CI // LANES
    rows = own + shared
    sizes = dict(rows=rows, nodes=nodes)
    shape = (3, rows, LANES)
    weight = jnp.pad(mass.reshape(1, own, LANES), ((0, 0), (0, shared), (0, 0)))
    partial_rhs = call(restrict_kernel, shape, fine_res, node_map, **sizes)
    residual = joined(lax.psum(partial_rhs, "grp"), own, shared)
    gamma = alpha = answer = direction = image = None
    for step in range(ITERS):
        forces = call(force_kernel, shape, residual, connect, grads, moduli, **sizes)
        forces = forces + weight * residual
        inner = residual[:, :own]
        sums = lax.psum(jnp.stack([jnp.sum(inner * inner), jnp.sum(residual * forces)]), "sub")
        last = step + 1 == ITERS
        applied = None if last else joined(forces, own, shared)
        if step == 0:
            alpha = sums[0] / sums[1]
            direction = residual
            image = applied
            answer = alpha * direction
        else:
            beta = sums[0] / gamma
            alpha = sums[0] / (sums[1] - beta * sums[0] / alpha)
            direction = residual + beta * direction
            answer = answer + alpha * direction
            if not last:
                image = applied + beta * image
        gamma = sums[0]
        if not last:
            residual = residual - alpha * image
    return call(prolong_kernel, fine_res.shape, answer, node_map, **sizes)


def solution(mesh):
    in_specs = (
        P(None, ("grp", "sub")),
        P(None, ("grp", "sub")),
        P(None, "sub"),
        P(None, None, "sub"),
        P(None, "sub"),
        P("sub"),
    )
    out_specs = P(None, ("grp", "sub"))
    return jax.shard_map(body, mesh=mesh, in_specs=in_specs, out_specs=out_specs, check_vma=False)
```
